32 devices in a mesh: dev: 8 (over z, x), rep: 4 (over y, core).
Axes of the slice: x: 2, y: 2, z: 4, core: 2. Of those that a mesh axis runs over, the one named last changes fastest.
Arguments:
- emb_table: float32 [32768, 160], P('dev'), may hold values from -6 to 6
- feature_ids: int32 [4096, 4, 8], P(('dev', 'rep')), may hold values from 0 to 8191
- lengths: int32 [4096, 4], P(('dev', 'rep')), may hold values from 1 to 8
- cotangent: float32 [4096, 4, 160], P(('dev', 'rep')), may hold values from -6 to 6
Outputs:
- pooled: float32 [4096, 4, 160], P(('dev', 'rep'))
- row_grads: float32 [32768, 160], P(('dev', 'rep'))
The draws below stay inside these ranges and needn't reach their ends.
All inputs are finite; a program needn't handle non-finite values.
Results may differ from the reference program's by a relative error of at most 0.00008.
Values sent between devices are 32-bit elements; how exact they have to be, the bound alone decides.
A program may use at most 128 MiB of HBM per device.

```python
import math
import jax
import jax.numpy as jnp
import numpy as np
from jax import lax

E = 160
FEATS = 4
BAG = 8
ROWS_DEV = 4096
ROWS = 32768
VOCAB = 8192
BATCH = 4096
N_DEV = 8


def touch_ends(entries, rng, low, largest):
    place = [jax.random.randint(jax.random.fold_in(rng, axis), (), 0, length) for axis, length in enumerate(entries.shape)]
    longest = entries.shape.index(max(entries.shape))
    beside = place[:longest] + [(place[longest] + 1) % entries.shape[longest]] + place[longest + 1:]
    return entries.at[tuple(place)].set(low).at[tuple(beside)].set(largest)


def steps_of(key, dims, pieces, smallest, high):
    loudness, own = 1.0, jax.random.fold_in(key, 6)
    for axis_at, blocks in pieces:
        draws = jnp.exp(jax.random.uniform(jax.random.fold_in(own, axis_at), (blocks,), jnp.float32, smallest / len(pieces), high / len(pieces)))
        loudness = loudness * jnp.repeat(draws, dims[axis_at] // blocks).reshape([-1 if axis == axis_at else 1 for axis in range(len(dims))])
    return loudness


def rank_table(amount, skew):
    loads = [(1 << 20) // math.isqrt(rank ** skew) + 1 for rank in range(1, amount + 1)]
    deviation = 1 + sum(loads) // (1 << 30)
    return np.cumsum(np.array([max(1, weight // deviation) for weight in loads]))


def ranked(stream_key, shape, count, lean):
    grid = rank_table(count, lean)
    ticket = jax.random.randint(jax.random.fold_in(stream_key, 1), shape, 0, int(grid[count - 1]))
    grade = jnp.searchsorted(jnp.asarray(grid, jnp.int32), ticket, side="right")
    return jax.random.permutation(jax.random.fold_in(stream_key, 2), count)[grade].astype(jnp.int32)


def centred(key, dims, deviation, limit, split=(), held_as=jnp.bfloat16):
    drawn = deviation * jax.random.normal(key, dims, jnp.float32)
    if split:
        drawn = drawn * steps_of(key, dims, split, -0.22, 0.18)
    return jnp.clip(drawn, -limit, limit).astype(held_as)


def setup_inputs(seed: int = 0) -> dict:
    key_list = jax.random.split(jax.random.key(seed), 5)
    return {
        "emb_table": centred(key_list[0], (ROWS, E), 1.0, 6.0, ((0, 8),), jnp.float32),
        "feature_ids": touch_ends(ranked(key_list[1], (BATCH, FEATS, BAG), VOCAB, 2), jax.random.fold_in(key_list[1], 3), 0, VOCAB - 1).astype(jnp.int32),
        "lengths": touch_ends(jax.random.randint(key_list[2], (BATCH, FEATS), 1, BAG + 1), jax.random.fold_in(key_list[2], 1), 1, BAG).astype(jnp.int32),
        "cotangent": centred(key_list[3], (BATCH, FEATS, E), 1.0, 6.0, ((0, 32),), jnp.float32),
    }


def reference(emb_table, feature_ids, lengths, cotangent):
    vocabulary = ROWS_DEV * N_DEV // FEATS
    slot_index = jnp.arange(BAG, dtype=jnp.int32)
    live_slots = slot_index[None, None, :] < lengths[:, :, None]
    share = 1.0 / lengths.astype(jnp.float32)
    weights = jnp.where(live_slots, share[:, :, None], 0.0).astype(jnp.float32)
    offsets = (jnp.arange(FEATS, dtype=jnp.int32) * vocabulary).astype(jnp.int32)
    global_ids = (feature_ids + offsets[None, :, None]).astype(jnp.int32)

    def pool_feature(inputs):
        feature_rows, feature_weights = inputs
        gathered = emb_table[feature_rows]
        return jnp.sum(gathered * feature_weights[:, :, None], axis=1)

    pooled = lax.map(pool_feature, (jnp.transpose(global_ids, (1, 0, 2)), jnp.transpose(weights, (1, 0, 2))))
    pooled = jnp.transpose(pooled, (1, 0, 2))

    def add_feature(running, inputs):
        feature_rows, feature_weights, feature_cot = inputs
        contrib = feature_weights[:, :, None] * feature_cot[:, None, :]
        running = running.at[feature_rows.reshape(-1)].add(contrib.reshape(-1, E))
        return running, None

    start_grads = jnp.zeros((ROWS_DEV * N_DEV, E), jnp.float32)
    row_grads, _ = lax.scan(add_feature, start_grads, (jnp.transpose(global_ids, (1, 0, 2)), jnp.transpose(weights, (1, 0, 2)), jnp.transpose(cotangent, (1, 0, 2))))
    return pooled, row_grads
```

```python
import functools

import jax
import jax.numpy as jnp
from jax import lax
from jax.experimental import pallas as pl
from jax.experimental.pallas import tpu as pltpu
from jax.sharding import PartitionSpec as P

F32, BF16, I32, I16 = jnp.float32, jnp.bfloat16, jnp.int32, jnp.int16
ROW_TILE = 256
INNER = 2


def split_bits(value):
    high = value.astype(BF16)
    low = (value - high.astype(F32)).astype(BF16)
    return high, low


def repeat(count, step):
    if count == 1:
        step(0)
    else:
        lax.fori_loop(0, count, lambda at, _: (step(at), 0)[1], 0)


def kernel(
    n, reps, table_in, ids_in, lens_in, cot_in, pool_in, grads, arrived,
    table, raw, lens, cot, ids, stage, ids_buf, peer_ids, cot_buf, peer_cot, counts, rest, halves, part, part_in,
    scaled, sums, total,
    id_send, id_recv, cot_send, cot_recv, pass_send, far_send, far_recv, far_id_send, far_id_recv,
    part_send, part_recv, pool_send, pool_recv, row_send, row_recv,
):
    features, bag, each = ids.shape
    width, rows_dev = table.shape
    owners = n // features
    outer = reps // INNER
    rows_out = rows_dev // reps
    kept = rows_out * INNER
    me = lax.axis_index("dev")
    rep = lax.axis_index("rep")
    feature = me // owners
    lane = me % owners
    group = rep // INNER
    core = rep % INNER
    first_row = group * kept
    bits = features.bit_length() - 1

    def crossed(step):
        value = feature
        for bit in range(bits):
            value = value + (step // (1 << bit) % 2) * (1 - 2 * (feature // (1 << bit) % 2)) * (1 << bit)
        return value

    def near(step):
        return (me + step) % n

    def beside(side):
        return feature * owners + (lane + side) % owners

    def across(step):
        return crossed(step) * owners + lane

    def source_of(step, side):
        return crossed(step) * owners + (lane + side) % owners

    def far(step):
        return (group + step) % outer * INNER + core

    partner = group * INNER + (core + 1) % INNER

    barrier = pltpu.get_barrier_semaphore()
    for step in range(1, n):
        pl.semaphore_signal(
            barrier, inc=1, device_id={"dev": near(step)}, device_id_type=pl.DeviceIdType.MESH
        )
    for step in range(1, outer):
        pl.semaphore_signal(
            barrier, inc=1, device_id={"rep": far(step)}, device_id_type=pl.DeviceIdType.MESH
        )
    pl.semaphore_signal(
        barrier, inc=1, device_id={"rep": partner}, device_id_type=pl.DeviceIdType.MESH
    )
    staged = [
        pltpu.make_async_copy(src, dst, stage.at[at])
        for at, (src, dst) in enumerate(
            ((ids_in, raw), (lens_in, lens), (cot_in, cot), (table_in, table))
        )
    ]
    for copy in staged:
        copy.start()
    staged[0].wait()
    staged[1].wait()
    slot_index = lax.broadcasted_iota(I32, (bag, each), 0)
    for at in range(features):
        ids[at] = jnp.where(slot_index < lens[at : at + 1], raw[at], -(1 << 20))
    staged[2].wait()
    ids_buf[me] = ids[feature]
    cot_buf[me] = cot[feature]
    pl.semaphore_wait(barrier, n - 1 + outer)

    def remote(src, dst, send, recv, axis, to):
        return pltpu.make_async_remote_copy(
            src_ref=src, dst_ref=dst, send_sem=send, recv_sem=recv,
            device_id={axis: to}, device_id_type=pl.DeviceIdType.MESH,
        )

    def id_copy(peer, source):
        return remote(
            ids.at[peer // owners], ids_buf.at[source],
            id_send.at[peer], id_recv.at[source], "dev", peer,
        )

    def cot_copy(peer, source):
        return remote(
            cot.at[peer // owners], cot_buf.at[source],
            cot_send.at[peer], cot_recv.at[source], "dev", peer,
        )

    def pass_copy(source, side):
        return remote(
            cot_buf.at[source], cot_buf.at[source],
            pass_send.at[source // owners, side], cot_recv.at[source], "dev", beside(side),
        )

    def far_copy(source, step, own=False):
        return remote(
            cot.at[feature] if own else cot_buf.at[source], peer_cot.at[step - 1, source],
            far_send.at[step - 1, source], far_recv.at[step - 1, source], "rep", far(step),
        )

    def far_id_copy(step):
        return remote(
            ids_buf, peer_ids.at[step - 1],
            far_id_send.at[step - 1], far_id_recv.at[step - 1], "rep", far(step),
        )

    def part_copy(source, slot):
        return remote(
            part.at[source], part_in.at[slot], part_send.at[source], part_recv.at[slot],
            "dev", feature * owners + source % owners,
        )

    def pool_copy(source, slot):
        return remote(
            part.at[source], pool_in.at[slot],
            pool_send.at[source // owners], pool_recv.at[slot], "dev", source,
        )

    for step in range(1, n):
        id_copy(near(step), me).start()
    for step in (1, 3, 2) if features == 4 else range(1, features):
        cot_copy(across(step), me).start()
    for side in range(1, owners):
        cot_copy(beside(side), me).start()
    for step in range(1, outer):
        far_copy(me, step, True).start()

    staged[3].wait()

    def split_table(tile):
        at = pl.ds(pl.multiple_of(tile * ROW_TILE, ROW_TILE), ROW_TILE)
        start = (first_row + tile * ROW_TILE) % rows_dev
        high, low = split_bits(table[:, pl.ds(pl.multiple_of(start, ROW_TILE), ROW_TILE)])
        halves[:width, at] = high
        halves[width:, at] = low

    repeat(rows_dev // ROW_TILE, split_table)

    def pass_on(step):
        source = across(step)
        cot_copy(source, source).wait_recv()
        for side in range(1, owners):
            pass_copy(source, side).start()
        for away in range(1, outer):
            far_copy(source, away).start()

    def send_far(step):
        for side in range(1, owners):
            source = source_of(step, side)
            cot_copy(source, source).wait_recv()
            for away in range(1, outer):
                far_copy(source, away).start()

    def slot_keys(blocks, rows):
        slots = jnp.concatenate(blocks, axis=1)
        wide = slots.shape[1]
        local = slots - lane * rows_dev
        turned = local - first_row
        turned = jnp.where(turned < 0, turned + rows_dev, turned)
        inside = (local >= 0) & (local < rows_dev) & (turned < rows)
        keys, times = [], []
        for j in range(bag):
            same = (slots == slots[j : j + 1]).astype(I32)
            count = jnp.sum(same, axis=0, keepdims=True)
            keep = inside[j : j + 1]
            if j:
                keep = keep & (jnp.sum(same[:j], axis=0, keepdims=True) == 0)
            key = jnp.where(keep, turned[j : j + 1], -1)
            keys.append(jnp.broadcast_to(key, (16, wide)).astype(I16))
            times.append(jnp.broadcast_to(count.astype(F32), (16, wide)).astype(BF16))
        return keys, times

    def count_rows(keys, times, start, rows, target, columns):
        wide = keys[0].shape[1]
        row = lax.broadcasted_iota(I32, (16, 128), 0)

        def count_tile(tile):
            at = pl.multiple_of(tile * ROW_TILE, ROW_TILE)
            base = row + (tile * ROW_TILE + start)
            for block in range(ROW_TILE // 16):
                here = (base + 16 * block).astype(I16)
                here = jnp.concatenate([here] * (wide // 128), axis=1)
                found = jnp.zeros((16, wide), BF16)
                for j in range(bag):
                    found = jnp.where(keys[j] == here, times[j], found)
                target[pl.ds(at + 16 * block, 16), columns] = found

        repeat(rows // ROW_TILE, count_tile)

    sides = owners // 2

    def pair_columns(step, pair):
        return pl.ds(pl.multiple_of((step * sides + pair) * 2 * each, 2 * each), 2 * each)

    def wait_ids(step):
        for side in range(owners):
            if step or side:
                source = source_of(step, side)
                id_copy(source, source).wait_recv()

    def count_pair(step, pair):
        blocks = [ids_buf[source_of(step, pair * 2 + half)] for half in range(2)]
        keys, times = slot_keys(blocks, rows_dev)
        columns = pair_columns(step, pair)
        count_rows(keys, times, 0, kept, counts, columns)
        count_rows(keys, times, kept, rows_dev - kept, rest, slice(None))

    def pool_pair(step, pair):
        columns = pair_columns(step, pair)
        both = jnp.dot(halves[:, :kept], counts[:, columns], preferred_element_type=F32)
        both = both + jnp.dot(halves[:, kept:], rest[...], preferred_element_type=F32)
        pool = both[:width] + both[width:]
        for half in range(2):
            side = pair * 2 + half
            source = source_of(step, side)
            part[source] = pool[:, half * each : (half + 1) * each]
            if isinstance(side, int):
                if side:
                    part_copy(source, source // owners * owners + lane).start()
            else:
                @pl.when(side > 0)
                def _():
                    part_copy(source, source // owners * owners + lane).start()

    def pools(step):
        def one(pair):
            count_pair(step, pair)
            pool_pair(step, pair)

        repeat(sides, one)

    def sum_parts(step):
        source = across(step)
        value = part[source]
        for side in range(1, owners):
            slot = source // owners * owners + (lane + side) % owners
            part_copy(source, slot).wait_recv()
            value = value + part_in[slot]
        if step:
            part[source] = value
            pool_copy(source, feature).start()
        else:
            pool_in[feature] = value

    def scale_block(live_ids, block, column):
        live = jnp.sum((live_ids >= 0).astype(F32), axis=0, keepdims=True)
        high, low = split_bits(block * (1.0 / live))
        columns = pl.ds(pl.multiple_of(column * each, each), each)
        scaled[:width, columns] = high
        scaled[width:, columns] = low

    def scale_own(step):
        def one(side):
            source = source_of(step, side)
            scale_block(ids_buf[source], cot_buf[source], step * owners + side)

        repeat(owners, one)

    def scale_far(away, step):
        for side in range(owners):
            source = source_of(step, side)
            far_copy(source, away).wait_recv()
            scale_block(peer_ids[away - 1, source], peer_cot[away - 1, source], away * n + step * owners + side)

    def count_far(away, step):
        def one(pair):
            blocks = [peer_ids[away - 1, source_of(step, pair * 2 + half)] for half in range(2)]
            keys, times = slot_keys(blocks, kept)
            count_rows(keys, times, 0, kept, counts, pair_columns(away * features + step, pair))

        repeat(sides, one)

    def grad_tile(start, low, high):
        rows = pl.ds(pl.multiple_of(start, ROW_TILE), ROW_TILE)
        both = lax.dot_general(
            scaled[:, low:high], counts[rows, low:high], (((1,), (1,)), ((), ())),
            preferred_element_type=F32,
        )
        return both[:width] + both[width:]

    def row_copy(tile):
        at = slice(tile * ROW_TILE, (tile + 1) * ROW_TILE)
        return remote(
            total.at[tile], arrived.at[tile], row_send.at[tile], row_recv.at[tile], "rep", partner,
        )

    wait_ids(0)
    pools(0)
    pass_on(1)
    send_far(0)
    for step in range(1, features):
        wait_ids(step)
    for away in range(1, outer):
        far_id_copy(away).start()
    pools(1)
    pass_on(2)
    send_far(1)
    sum_parts(0)
    pools(2)
    sum_parts(1)
    pass_on(3)
    send_far(2)
    pools(3)
    sum_parts(2)
    send_far(3)
    for step in range(features):
        scale_own(step)
    for away in range(1, outer):
        far_id_copy(away).wait_recv()
        for step in range(features):
            count_far(away, step)
            if step == 1 and away == 1:
                sum_parts(3)
    middle = scaled.shape[1] - 2 * owners * each
    for away in range(1, outer):
        for step in range(features - 2 if away == outer - 1 else features):
            scale_far(away, step)

    def add_early(tile):
        columns = pl.ds(pl.multiple_of(tile * ROW_TILE, ROW_TILE), ROW_TILE)
        sums[:, columns] = grad_tile(tile * ROW_TILE, 0, middle)

    repeat(kept // ROW_TILE, add_early)
    for step in range(features - 2, features):
        scale_far(outer - 1, step)
    tiles = rows_out // ROW_TILE
    for tile in range(tiles):
        start = pl.multiple_of((core + 1) % INNER * rows_out + tile * ROW_TILE, ROW_TILE)
        total[tile] = grad_tile(start, middle, scaled.shape[1]) + sums[:, pl.ds(start, ROW_TILE)]
        row_copy(tile).start()
    for tile in range(tiles):
        start = pl.multiple_of(core * rows_out + tile * ROW_TILE, ROW_TILE)
        grads[tile] = grad_tile(start, middle, scaled.shape[1]) + sums[:, pl.ds(start, ROW_TILE)]
    for step in range(1, features):
        pool_copy(across(step), crossed(step)).wait_recv()
    for tile in range(tiles):
        row_copy(tile).wait_recv()

    for tile in range(tiles):
        row_copy(tile).wait_send()
    for step in range(1, n):
        id_copy(near(step), me).wait_send()
    for side in range(1, owners):
        cot_copy(beside(side), me).wait_send()
    for away in range(1, outer):
        far_id_copy(away).wait_send()
        far_copy(me, away, True).wait_send()
    for step in range(features):
        source = across(step)
        if step:
            cot_copy(source, me).wait_send()
            pool_copy(source, feature).wait_send()
            for away in range(1, outer):
                far_copy(source, away).wait_send()
        for side in range(1, owners):
            if step:
                pass_copy(source, side).wait_send()
            other = source_of(step, side)
            for away in range(1, outer):
                far_copy(other, away).wait_send()
            part_copy(other, crossed(step) * owners + lane).wait_send()


def finish(lens, pool, own, arrived, pooled, grads):
    for at in range(pool.shape[0]):
        pooled[at] = pool[at] * (1.0 / lens[at : at + 1].astype(F32))
    for tile in range(own.shape[0]):
        grads[:, tile * ROW_TILE : (tile + 1) * ROW_TILE] = own[tile] + arrived[tile]


def body(n, reps, emb_table, feature_ids, lengths, cotangent):
    rows_dev, width = emb_table.shape
    each, features, bag = feature_ids.shape
    lens = lengths.T
    owners = n // features
    outer = reps // INNER
    rows_out = rows_dev // reps
    kept = rows_out * INNER
    tiles = rows_out // ROW_TILE
    away = max(outer - 1, 1)
    sem = pltpu.SemaphoreType.DMA
    vmem = pl.BlockSpec(memory_space=pltpu.VMEM)
    pool_shape = jax.ShapeDtypeStruct((features, width, each), F32)
    tile_shape = jax.ShapeDtypeStruct((tiles, width, ROW_TILE), F32)
    pool, own, arrived = pl.pallas_call(
        functools.partial(kernel, n, reps),
        out_shape=(pool_shape, tile_shape, tile_shape),
        in_specs=[pl.BlockSpec(memory_space=pl.ANY)] * 4,
        out_specs=[vmem] * 3,
        scratch_shapes=[
            pltpu.VMEM((width, rows_dev), F32),
            pltpu.VMEM((features, bag, each), I32),
            pltpu.VMEM((features, each), I32),
            pltpu.VMEM((features, width, each), F32),
            pltpu.VMEM((features, bag, each), I32),
            sem((4,)),
            pltpu.VMEM((n, bag, each), I32),
            pltpu.VMEM((away, n, bag, each), I32),
            pltpu.VMEM((n, width, each), F32),
            pltpu.VMEM((away, n, width, each), F32),
            pltpu.VMEM((kept, outer * n * each), BF16),
            pltpu.VMEM((rows_dev - kept, 2 * each), BF16),
            pltpu.VMEM((2 * width, rows_dev), BF16),
            pltpu.VMEM((n, width, each), F32),
            pltpu.VMEM((n, width, each), F32),
            pltpu.VMEM((2 * width, outer * n * each), BF16),
            pltpu.VMEM((width, kept), F32),
            pltpu.VMEM((tiles, width, ROW_TILE), F32),
            sem((n,)), sem((n,)), sem((n,)), sem((n,)), sem((features, owners)),
            sem((away, n)), sem((away, n)), sem((away,)), sem((away,)),
            sem((n,)), sem((n,)), sem((features,)), sem((features,)),
            sem((tiles,)), sem((tiles,)),
        ],
        compiler_params=pltpu.CompilerParams(
            collective_id=0, has_side_effects=True, vmem_limit_bytes=60 * 1024 * 1024
        ),
    )(
        emb_table.T, jnp.transpose(feature_ids, (1, 2, 0)), lens,
        jnp.transpose(cotangent, (1, 2, 0)),
    )
    pooled, grads = pl.pallas_call(
        finish,
        out_shape=(pool_shape, jax.ShapeDtypeStruct((width, rows_out), F32)),
        in_specs=[vmem] * 4,
        out_specs=[vmem] * 2,
    )(lens, pool, own, arrived)
    return jnp.transpose(pooled, (2, 0, 1)), grads.T


def solution(mesh):
    return jax.shard_map(
        functools.partial(body, mesh.shape["dev"], mesh.shape["rep"]),
        mesh=mesh,
        in_specs=(
            P("dev", None),
            P(("dev", "rep"), None, None),
            P(("dev", "rep"), None),
            P(("dev", "rep"), None, None),
        ),
        out_specs=(P(("dev", "rep"), None, None), P(("dev", "rep"), None)),
        check_vma=False,
    )
```

```python
import functools

import jax
import jax.numpy as jnp
from jax import lax
from jax.experimental import pallas as pl
from jax.experimental.pallas import tpu as pltpu
from jax.sharding import PartitionSpec as P

F32, BF16, I32, I16 = jnp.float32, jnp.bfloat16, jnp.int32, jnp.int16
ROW_TILE = 256
BLOCK = 64
INNER = 2


def split_bits(value):
    high = value.astype(BF16)
    low = (value - high.astype(F32)).astype(BF16)
    return high, low


def repeat(count, step):
    if count == 1:
        step(0)
    else:
        lax.fori_loop(0, count, lambda at, _: (step(at), 0)[1], 0)


def kernel(
    n, reps, table_in, ids_in, lens_in, cot_in, pool_in, grads, arrived,
    table, raw, lens, cot, ids, stage, ids_buf, peer_ids, cot_buf, peer_cot, halves, part, part_in,
    scaled, sums, total,
    id_send, id_recv, cot_send, cot_recv, pass_send, far_send, far_recv, far_id_send, far_id_recv,
    part_send, part_recv, pool_send, pool_recv, row_send, row_recv, *counted,
):
    features, bag, each = ids.shape
    width, rows_dev = table.shape
    owners = n // features
    outer = reps // INNER
    rows_out = rows_dev // reps
    kept = rows_out * INNER
    me = lax.axis_index("dev")
    rep = lax.axis_index("rep")
    feature = me // owners
    lane = me % owners
    group = rep // INNER
    core = rep % INNER
    first_row = group * kept
    sides = owners // 2
    counts, rests = counted[: outer * n // 2], counted[outer * n // 2 :]
    bits = features.bit_length() - 1

    def crossed(step):
        value = feature
        for bit in range(bits):
            value = value + (step // (1 << bit) % 2) * (1 - 2 * (feature // (1 << bit) % 2)) * (1 << bit)
        return value

    def near(step):
        return (me + step) % n

    def beside(side):
        return feature * owners + (lane + side) % owners

    def across(step):
        return crossed(step) * owners + lane

    def source_of(step, side):
        return crossed(step) * owners + (lane + side) % owners

    def far(step):
        return (group + step) % outer * INNER + core

    partner = group * INNER + (core + 1) % INNER

    barrier = pltpu.get_barrier_semaphore()
    for step in range(1, n):
        pl.semaphore_signal(
            barrier, inc=1, device_id={"dev": near(step)}, device_id_type=pl.DeviceIdType.MESH
        )
    for step in range(1, outer):
        pl.semaphore_signal(
            barrier, inc=1, device_id={"rep": far(step)}, device_id_type=pl.DeviceIdType.MESH
        )
    pl.semaphore_signal(
        barrier, inc=1, device_id={"rep": partner}, device_id_type=pl.DeviceIdType.MESH
    )
    staged = [
        pltpu.make_async_copy(src, dst, stage.at[at])
        for at, (src, dst) in enumerate(
            ((ids_in, raw), (lens_in, lens), (cot_in, cot), (table_in, table))
        )
    ]
    for copy in staged:
        copy.start()
    staged[0].wait()
    staged[1].wait()
    slot_index = lax.broadcasted_iota(I32, (bag, each), 0)
    for at in range(features):
        ids[at] = jnp.where(slot_index < lens[at : at + 1], raw[at], -(1 << 20))
    staged[2].wait()
    ids_buf[me] = ids[feature]
    cot_buf[me] = cot[feature]
    pl.semaphore_wait(barrier, n - 1 + outer)

    def remote(src, dst, send, recv, axis, to):
        return pltpu.make_async_remote_copy(
            src_ref=src, dst_ref=dst, send_sem=send, recv_sem=recv,
            device_id={axis: to}, device_id_type=pl.DeviceIdType.MESH,
        )

    def id_copy(peer, source):
        return remote(
            ids.at[peer // owners], ids_buf.at[source],
            id_send.at[peer], id_recv.at[source], "dev", peer,
        )

    def cot_copy(peer, source):
        return remote(
            cot.at[peer // owners], cot_buf.at[source],
            cot_send.at[peer], cot_recv.at[source], "dev", peer,
        )

    def pass_copy(source, side):
        return remote(
            cot_buf.at[source], cot_buf.at[source],
            pass_send.at[source // owners, side], cot_recv.at[source], "dev", beside(side),
        )

    def far_copy(source, step, own=False):
        return remote(
            cot.at[feature] if own else cot_buf.at[source], peer_cot.at[step - 1, source],
            far_send.at[step - 1, source], far_recv.at[step - 1, source], "rep", far(step),
        )

    def far_id_copy(step):
        return remote(
            ids_buf, peer_ids.at[step - 1],
            far_id_send.at[step - 1], far_id_recv.at[step - 1], "rep", far(step),
        )

    def part_copy(source, slot):
        return remote(
            part.at[source], part_in.at[slot], part_send.at[source], part_recv.at[slot],
            "dev", feature * owners + source % owners,
        )

    def pool_copy(source, slot):
        return remote(
            part.at[source], pool_in.at[slot],
            pool_send.at[source // owners], pool_recv.at[slot], "dev", source,
        )

    for step in range(1, n):
        id_copy(near(step), me).start()
    for step in (1, 3, 2) if features == 4 else range(1, features):
        cot_copy(across(step), me).start()
    for side in range(1, owners):
        cot_copy(beside(side), me).start()
    for step in range(1, outer):
        far_copy(me, step, True).start()

    staged[3].wait()

    def split_table(tile):
        at = pl.ds(pl.multiple_of(tile * ROW_TILE, ROW_TILE), ROW_TILE)
        start = (first_row + tile * ROW_TILE) % rows_dev
        high, low = split_bits(table[:, pl.ds(pl.multiple_of(start, ROW_TILE), ROW_TILE)])
        halves[:width, at] = high
        halves[width:, at] = low

    repeat(rows_dev // ROW_TILE, split_table)

    def pass_on(step):
        source = across(step)
        cot_copy(source, source).wait_recv()
        for side in range(1, owners):
            pass_copy(source, side).start()
        for away in range(1, outer):
            far_copy(source, away).start()

    def send_far(step):
        for side in range(1, owners):
            source = source_of(step, side)
            cot_copy(source, source).wait_recv()
            for away in range(1, outer):
                far_copy(source, away).start()

    def slot_keys(blocks, rows):
        slots = jnp.concatenate(blocks, axis=1)
        wide = slots.shape[1]
        local = slots - lane * rows_dev
        turned = local - first_row
        turned = jnp.where(turned < 0, turned + rows_dev, turned)
        inside = (local >= 0) & (local < rows_dev) & (turned < rows)
        keys, times = [], []
        for j in range(bag):
            same = (slots == slots[j : j + 1]).astype(I32)
            count = jnp.sum(same, axis=0, keepdims=True)
            keep = inside[j : j + 1]
            if j:
                keep = keep & (jnp.sum(same[:j], axis=0, keepdims=True) == 0)
            key = jnp.where(keep, turned[j : j + 1], -1)
            keys.append(jnp.broadcast_to(key, (16, wide)).astype(I16))
            times.append(jnp.broadcast_to(count.astype(F32), (16, wide)).astype(BF16))
        return keys, times

    def count_rows(keys, times, start, rows, target):
        wide = keys[0].shape[1]
        lanes = wide // 128
        row = lax.broadcasted_iota(I32, (16, 128), 0)
        spread = BLOCK // 16
        keys = [jnp.concatenate([key] * spread, axis=0) for key in keys]
        times = [jnp.concatenate([time] * spread, axis=0) for time in times]
        for block in range(rows // BLOCK):
            first = start + block * BLOCK
            here = [(row + (first + 16 * at)).astype(I16) for at in range(spread)]
            here = jnp.concatenate([jnp.concatenate([one] * lanes, axis=1) for one in here], axis=0)
            found = jnp.zeros((BLOCK, wide), BF16)
            for key, time in zip(keys, times):
                found = jnp.where(key == here, time, found)
            target[block * BLOCK : (block + 1) * BLOCK, :] = found

    def wait_ids(step):
        for side in range(owners):
            if step or side:
                source = source_of(step, side)
                id_copy(source, source).wait_recv()

    def pair_at(step, pair, away=0):
        return (away * features + step) * sides + pair

    def count_pair(step, pair):
        at = pair_at(step, pair)
        keys, times = slot_keys([ids_buf[source_of(step, pair * 2 + half)] for half in range(2)], rows_dev)
        count_rows(keys, times, 0, kept, counts[at])
        count_rows(keys, times, kept, rows_dev - kept, rests[at % 2])

    def pool_pair(step, pair):
        at = pair_at(step, pair)
        pool = jnp.dot(halves[:, :kept], counts[at][...], preferred_element_type=F32)
        pool = pool + jnp.dot(halves[:, kept:], rests[at % 2][...], preferred_element_type=F32)
        pool = pool[:width] + pool[width:]
        for half in range(2):
            side = pair * 2 + half
            source = source_of(step, side)
            part[source] = pool[:, half * each : (half + 1) * each]
            if side:
                part_copy(source, source // owners * owners + lane).start()

    def count_far(step, away=1):
        for pair in range(sides):
            blocks = [peer_ids[away - 1, source_of(step, pair * 2 + half)] for half in range(2)]
            keys, times = slot_keys(blocks, kept)
            count_rows(keys, times, 0, kept, counts[pair_at(step, pair, away)])

    def sum_parts(step):
        source = across(step)
        value = part[source]
        for side in range(1, owners):
            slot = source // owners * owners + (lane + side) % owners
            part_copy(source, slot).wait_recv()
            value = value + part_in[slot]
        if step:
            part[source] = value
            pool_copy(source, feature).start()
        else:
            pool_in[feature] = value

    def scale_block(live_ids, block, column):
        live = jnp.sum((live_ids >= 0).astype(F32), axis=0, keepdims=True)
        high, low = split_bits(block * (1.0 / live))
        columns = pl.ds(pl.multiple_of(column * each, each), each)
        scaled[:width, columns] = high
        scaled[width:, columns] = low

    def scale_own(step):
        def one(side):
            source = source_of(step, side)
            scale_block(ids_buf[source], cot_buf[source], step * owners + side)

        repeat(owners, one)

    def scale_far(away, step):
        for side in range(owners):
            source = source_of(step, side)
            far_copy(source, away).wait_recv()
            scale_block(peer_ids[away - 1, source], peer_cot[away - 1, source], away * n + step * owners + side)

    def grad_rows(start, rows, low, high):
        at = pl.ds(pl.multiple_of(start, ROW_TILE), rows)
        held = jnp.concatenate([counts[pair][at, :] for pair in range(low, high)], axis=1)
        both = lax.dot_general(
            scaled[:, low * 2 * each : high * 2 * each], held, (((1,), (1,)), ((), ())),
            preferred_element_type=F32,
        )
        return both[:width] + both[width:]

    def row_copy(tile):
        at = slice(tile * ROW_TILE, (tile + 1) * ROW_TILE)
        return remote(
            total.at[tile], arrived.at[tile], row_send.at[tile], row_recv.at[tile], "rep", partner,
        )

    order = list(range(1, features)) + [0]
    last = order[-1]
    before = None
    for place, step in enumerate(order):
        for pair in range(sides):
            if pair == 0 and place == 0:
                wait_ids(step)
            count_pair(step, pair)
            if before is not None:
                pool_pair(*before)
            before = step, pair
        if place == 0:
            pass_on(1)
            send_far(0)
            for other in order[1:]:
                wait_ids(other)
            for away in range(1, outer):
                far_id_copy(away).start()
        if place == 2:
            pass_on(2)
            send_far(1)
        if place == features - 1:
            pass_on(3)
            sum_parts(1)
    pool_pair(*before)
    for away in range(1, outer):
        far_id_copy(away).wait_recv()
        for step in range(features):
            count_far(step, away)
            if away == 1 and step == 1:
                send_far(2)
                sum_parts(2)
    for step in range(3):
        scale_own(step)
    send_far(3)
    scale_own(3)
    sum_parts(3)
    for away in range(1, outer):
        for step in range(features - 2 if away == outer - 1 else features):
            scale_far(away, step)
    pairs = outer * n // 2
    middle = pairs - 2 * sides
    for half in range(2):
        start = half * rows_out
        sums[:, start : start + rows_out] = grad_rows(start, rows_out, 0, middle)
    for step in range(features - 2, features):
        scale_far(outer - 1, step)
    tiles = rows_out // ROW_TILE
    start = pl.multiple_of((core + 1) % INNER * rows_out, ROW_TILE)
    value = grad_rows(start, rows_out, middle, pairs) + sums[:, pl.ds(start, rows_out)]
    for tile in range(tiles):
        total[tile] = value[:, tile * ROW_TILE : (tile + 1) * ROW_TILE]
        row_copy(tile).start()
    start = pl.multiple_of(core * rows_out, ROW_TILE)
    value = grad_rows(start, rows_out, middle, pairs) + sums[:, pl.ds(start, rows_out)]
    for tile in range(tiles):
        grads[tile] = value[:, tile * ROW_TILE : (tile + 1) * ROW_TILE]
    sum_parts(0)
    for step in range(1, features):
        pool_copy(across(step), crossed(step)).wait_recv()
    for tile in range(tiles):
        row_copy(tile).wait_recv()

    for tile in range(tiles):
        row_copy(tile).wait_send()
    for step in range(1, n):
        id_copy(near(step), me).wait_send()
    for side in range(1, owners):
        cot_copy(beside(side), me).wait_send()
    for away in range(1, outer):
        far_id_copy(away).wait_send()
        far_copy(me, away, True).wait_send()
    for step in range(features):
        source = across(step)
        if step:
            cot_copy(source, me).wait_send()
            pool_copy(source, feature).wait_send()
            for away in range(1, outer):
                far_copy(source, away).wait_send()
        for side in range(1, owners):
            if step:
                pass_copy(source, side).wait_send()
            other = source_of(step, side)
            for away in range(1, outer):
                far_copy(other, away).wait_send()
            part_copy(other, crossed(step) * owners + lane).wait_send()


def finish(lens, pool, own, arrived, pooled, grads):
    for at in range(pool.shape[0]):
        pooled[at] = pool[at] * (1.0 / lens[at : at + 1].astype(F32))
    for tile in range(own.shape[0]):
        grads[:, tile * ROW_TILE : (tile + 1) * ROW_TILE] = own[tile] + arrived[tile]


def body(n, reps, emb_table, feature_ids, lengths, cotangent):
    rows_dev, width = emb_table.shape
    each, features, bag = feature_ids.shape
    lens = lengths.T
    owners = n // features
    outer = reps // INNER
    rows_out = rows_dev // reps
    kept = rows_out * INNER
    tiles = rows_out // ROW_TILE
    away = max(outer - 1, 1)
    sem = pltpu.SemaphoreType.DMA
    vmem = pl.BlockSpec(memory_space=pltpu.VMEM)
    pool_shape = jax.ShapeDtypeStruct((features, width, each), F32)
    tile_shape = jax.ShapeDtypeStruct((tiles, width, ROW_TILE), F32)
    pool, own, arrived = pl.pallas_call(
        functools.partial(kernel, n, reps),
        out_shape=(pool_shape, tile_shape, tile_shape),
        in_specs=[pl.BlockSpec(memory_space=pl.ANY)] * 4,
        out_specs=[vmem] * 3,
        scratch_shapes=[
            pltpu.VMEM((width, rows_dev), F32),
            pltpu.VMEM((features, bag, each), I32),
            pltpu.VMEM((features, each), I32),
            pltpu.VMEM((features, width, each), F32),
            pltpu.VMEM((features, bag, each), I32),
            sem((4,)),
            pltpu.VMEM((n, bag, each), I32),
            pltpu.VMEM((away, n, bag, each), I32),
            pltpu.VMEM((n, width, each), F32),
            pltpu.VMEM((away, n, width, each), F32),
            pltpu.VMEM((2 * width, rows_dev), BF16),
            pltpu.VMEM((n, width, each), F32),
            pltpu.VMEM((n, width, each), F32),
            pltpu.VMEM((2 * width, outer * n * each), BF16),
            pltpu.VMEM((width, kept), F32),
            pltpu.VMEM((tiles, width, ROW_TILE), F32),
            sem((n,)), sem((n,)), sem((n,)), sem((n,)), sem((features, owners)),
            sem((away, n)), sem((away, n)), sem((away,)), sem((away,)),
            sem((n,)), sem((n,)), sem((features,)), sem((features,)),
            sem((tiles,)), sem((tiles,)),
        ]
        + [pltpu.VMEM((kept, 2 * each), BF16)] * (outer * n // 2)
        + [pltpu.VMEM((rows_dev - kept, 2 * each), BF16)] * 2,
        compiler_params=pltpu.CompilerParams(
            collective_id=0, has_side_effects=True, vmem_limit_bytes=60 * 1024 * 1024
        ),
    )(
        emb_table.T, jnp.transpose(feature_ids, (1, 2, 0)), lens,
        jnp.transpose(cotangent, (1, 2, 0)),
    )
    pooled, grads = pl.pallas_call(
        finish,
        out_shape=(pool_shape, jax.ShapeDtypeStruct((width, rows_out), F32)),
        in_specs=[vmem] * 4,
        out_specs=[vmem] * 2,
    )(lens, pool, own, arrived)
    return jnp.transpose(pooled, (2, 0, 1)), grads.T


def solution(mesh):
    return jax.shard_map(
        functools.partial(body, mesh.shape["dev"], mesh.shape["rep"]),
        mesh=mesh,
        in_specs=(
            P("dev", None),
            P(("dev", "rep"), None, None),
            P(("dev", "rep"), None),
            P(("dev", "rep"), None, None),
        ),
        out_specs=(P(("dev", "rep"), None, None), P(("dev", "rep"), None)),
        check_vma=False,
    )
```

```python
import functools
import math

import jax
import jax.numpy as jnp
from jax import lax
from jax.experimental import pallas as pl
from jax.experimental.pallas import tpu as pltpu
from jax.sharding import PartitionSpec as P

F32, BF16, I32, I16 = jnp.float32, jnp.bfloat16, jnp.int32, jnp.int16
ROW_TILE = 256
BLOCK = 64
CHUNK = 512
INNER = 2


def split_bits(value):
    high = value.astype(BF16)
    low = (value - high.astype(F32)).astype(BF16)
    return high, low


def repeat(count, step):
    if count == 1:
        step(0)
    else:
        lax.fori_loop(0, count, lambda at, _: (step(at), 0)[1], 0)


def kernel(
    n, reps, table_in, ids_in, lens_in, cot_in, pool_in, grads, arrived,
    table, raw, lens, cot, ids, stage, ids_buf, peer_ids, cot_buf, peer_cot, halves, part, part_in,
    scaled, sums, total,
    id_send, id_recv, cot_send, cot_recv, pass_send, far_send, far_recv, far_id_send, far_id_recv,
    part_send, part_recv, pool_send, pool_recv, row_send, row_recv, *counted,
):
    features, bag, each = ids.shape
    width, rows_dev = table.shape
    owners = n // features
    outer = reps // INNER
    rows_out = rows_dev // reps
    kept = rows_out * INNER
    me = lax.axis_index("dev")
    rep = lax.axis_index("rep")
    feature = me // owners
    lane = me % owners
    group = rep // INNER
    core = rep % INNER
    first_row = group * kept
    sides = owners // 2
    counts, rests = counted[: outer * n // 2], counted[outer * n // 2 :]
    bits = features.bit_length() - 1

    def crossed(step):
        value = feature
        for bit in range(bits):
            value = value + (step // (1 << bit) % 2) * (1 - 2 * (feature // (1 << bit) % 2)) * (1 << bit)
        return value

    def near(step):
        return (me + step) % n

    def beside(side):
        return feature * owners + (lane + side) % owners

    def across(step):
        return crossed(step) * owners + lane

    def source_of(step, side):
        return crossed(step) * owners + (lane + side) % owners

    def far(step):
        return (group + step) % outer * INNER + core

    partner = group * INNER + (core + 1) % INNER

    barrier = pltpu.get_barrier_semaphore()
    for step in range(1, n):
        pl.semaphore_signal(
            barrier, inc=1, device_id={"dev": near(step)}, device_id_type=pl.DeviceIdType.MESH
        )
    for step in range(1, outer):
        pl.semaphore_signal(
            barrier, inc=1, device_id={"rep": far(step)}, device_id_type=pl.DeviceIdType.MESH
        )
    pl.semaphore_signal(
        barrier, inc=1, device_id={"rep": partner}, device_id_type=pl.DeviceIdType.MESH
    )
    staged = [
        pltpu.make_async_copy(src, dst, stage.at[at])
        for at, (src, dst) in enumerate(
            ((ids_in, raw), (lens_in, lens), (cot_in, cot), (table_in, table))
        )
    ]
    for copy in staged:
        copy.start()
    staged[0].wait()
    staged[1].wait()
    slot_index = lax.broadcasted_iota(I32, (bag, each), 0)
    for at in range(features):
        ids[at] = jnp.where(slot_index < lens[at : at + 1], raw[at], -(1 << 20))
    staged[2].wait()
    ids_buf[me] = ids[feature]
    cot_buf[me] = cot[feature]
    pl.semaphore_wait(barrier, n - 1 + outer)

    def remote(src, dst, send, recv, axis, to):
        return pltpu.make_async_remote_copy(
            src_ref=src, dst_ref=dst, send_sem=send, recv_sem=recv,
            device_id={axis: to}, device_id_type=pl.DeviceIdType.MESH,
        )

    def id_copy(peer, source):
        return remote(
            ids.at[peer // owners], ids_buf.at[source],
            id_send.at[peer], id_recv.at[source], "dev", peer,
        )

    def cot_copy(peer, source):
        return remote(
            cot.at[peer // owners], cot_buf.at[source],
            cot_send.at[peer], cot_recv.at[source], "dev", peer,
        )

    def pass_copy(source, side):
        return remote(
            cot_buf.at[source], cot_buf.at[source],
            pass_send.at[source // owners, side], cot_recv.at[source], "dev", beside(side),
        )

    def far_copy(source, step, own=False):
        return remote(
            cot.at[feature] if own else cot_buf.at[source], peer_cot.at[step - 1, source],
            far_send.at[step - 1, source], far_recv.at[step - 1, source], "rep", far(step),
        )

    def far_id_copy(step):
        return remote(
            ids_buf, peer_ids.at[step - 1],
            far_id_send.at[step - 1], far_id_recv.at[step - 1], "rep", far(step),
        )

    def part_copy(source, slot):
        return remote(
            part.at[source], part_in.at[slot], part_send.at[source], part_recv.at[slot],
            "dev", feature * owners + source % owners,
        )

    def pool_copy(source, slot):
        return remote(
            part.at[source], pool_in.at[slot],
            pool_send.at[source // owners], pool_recv.at[slot], "dev", source,
        )

    for step in range(1, n):
        id_copy(near(step), me).start()
    for step in (1, 3, 2) if features == 4 else range(1, features):
        cot_copy(across(step), me).start()
    for side in range(1, owners):
        cot_copy(beside(side), me).start()
    for step in range(1, outer):
        far_copy(me, step, True).start()

    staged[3].wait()

    def split_table(tile):
        at = pl.ds(pl.multiple_of(tile * ROW_TILE, ROW_TILE), ROW_TILE)
        start = (first_row + tile * ROW_TILE) % rows_dev
        high, low = split_bits(table[:, pl.ds(pl.multiple_of(start, ROW_TILE), ROW_TILE)])
        halves[:width, at] = high
        halves[width:, at] = low

    repeat(rows_dev // ROW_TILE, split_table)

    def pass_on(step):
        source = across(step)
        cot_copy(source, source).wait_recv()
        for side in range(1, owners):
            pass_copy(source, side).start()
        for away in range(1, outer):
            far_copy(source, away).start()

    def send_far(step):
        for side in range(1, owners):
            source = source_of(step, side)
            cot_copy(source, source).wait_recv()
            for away in range(1, outer):
                far_copy(source, away).start()

    def slot_keys(blocks, rows):
        slots = jnp.concatenate(blocks, axis=1)
        wide = slots.shape[1]
        local = slots - lane * rows_dev
        turned = local - first_row
        turned = jnp.where(turned < 0, turned + rows_dev, turned)
        inside = (local >= 0) & (local < rows_dev) & (turned < rows)
        keys, times = [], []
        for j in range(bag):
            same = (slots == slots[j : j + 1]).astype(I32)
            count = jnp.sum(same, axis=0, keepdims=True)
            keep = inside[j : j + 1]
            if j:
                keep = keep & (jnp.sum(same[:j], axis=0, keepdims=True) == 0)
            key = jnp.where(keep, turned[j : j + 1], -1)
            keys.append(jnp.broadcast_to(key, (16, wide)).astype(I16))
            times.append(jnp.broadcast_to(count.astype(F32), (16, wide)).astype(BF16))
        return keys, times

    def count_rows(keys, times, start, first, rows, target):
        wide = keys[0].shape[1]
        lanes = wide // 128
        row = lax.broadcasted_iota(I32, (16, 128), 0)
        spread = BLOCK // 16
        keys = [jnp.concatenate([key] * spread, axis=0) for key in keys]
        times = [jnp.concatenate([time] * spread, axis=0) for time in times]
        for block in range(first // BLOCK, (first + rows) // BLOCK):
            base = start + block * BLOCK
            here = [(row + (base + 16 * at)).astype(I16) for at in range(spread)]
            here = jnp.concatenate([jnp.concatenate([one] * lanes, axis=1) for one in here], axis=0)
            found = jnp.zeros((BLOCK, wide), BF16)
            for key, time in zip(keys, times):
                found = jnp.where(key == here, time, found)
            target[block * BLOCK : (block + 1) * BLOCK, :] = found

    def wait_ids(step):
        for side in range(owners):
            if step or side:
                source = source_of(step, side)
                id_copy(source, source).wait_recv()

    def pair_at(step, pair, away=0):
        return (away * features + step) * sides + pair

    def keys_of(step, pair):
        return slot_keys([ids_buf[source_of(step, pair * 2 + half)] for half in range(2)], rows_dev)

    def halves_of(at):
        return (counts[at], 0, kept), (rests[at % 2], kept, rows_dev - kept)

    def stage(new, old, whiches=(0, 1)):
        if new is not None:
            keys, times = keys_of(*new)
        pool = None
        for which in whiches:
            rows = (kept, rows_dev - kept)[which]
            for first in range(0, rows, CHUNK):
                if old is not None:
                    target, start, _ = halves_of(pair_at(*old))[which]
                    piece = jnp.dot(
                        halves[:, start + first : start + first + CHUNK], target[first : first + CHUNK, :],
                        preferred_element_type=F32,
                    )
                    pool = piece if pool is None else pool + piece
                if new is not None:
                    target, start, _ = halves_of(pair_at(*new))[which]
                    count_rows(keys, times, start, first, CHUNK, target)
        if old is not None:
            step, pair = old
            pool = pool[:width] + pool[width:]
            for half in range(2):
                source = source_of(step, pair * 2 + half)
                value = pool[:, half * each : (half + 1) * each]
                part[source] = value if 0 in whiches else part[source] + value

    def start_parts(step):
        for side in range(1, owners):
            source = source_of(step, side)
            part_copy(source, source // owners * owners + lane).start()

    def count_far(step, away=1):
        for pair in range(sides):
            blocks = [peer_ids[away - 1, source_of(step, pair * 2 + half)] for half in range(2)]
            keys, times = slot_keys(blocks, kept)
            count_rows(keys, times, 0, 0, kept, counts[pair_at(step, pair, away)])

    def sum_parts(step):
        source = across(step)
        value = part[source]
        for side in range(1, owners):
            slot = source // owners * owners + (lane + side) % owners
            part_copy(source, slot).wait_recv()
            value = value + part_in[slot]
        if step:
            part[source] = value
            pool_copy(source, feature).start()
        else:
            pool_in[feature] = value

    def scale_block(live_ids, block, column):
        live = jnp.sum((live_ids >= 0).astype(F32), axis=0, keepdims=True)
        high, low = split_bits(block * (1.0 / live))
        columns = pl.ds(pl.multiple_of(column * each, each), each)
        scaled[:width, columns] = high
        scaled[width:, columns] = low

    def scale_own(step):
        def one(side):
            source = source_of(step, side)
            scale_block(ids_buf[source], cot_buf[source], step * owners + side)

        repeat(owners, one)

    def scale_far(away, step):
        for side in range(owners):
            source = source_of(step, side)
            far_copy(source, away).wait_recv()
            scale_block(peer_ids[away - 1, source], peer_cot[away - 1, source], away * n + step * owners + side)

    def grad_rows(start, rows, pairs):
        at = pl.ds(pl.multiple_of(start, ROW_TILE), rows)
        left = jnp.concatenate([scaled[:, pair * 2 * each : (pair + 1) * 2 * each] for pair in pairs], axis=1)
        held = jnp.concatenate([counts[pair][at, :] for pair in pairs], axis=1)
        both = lax.dot_general(
            left, held, (((1,), (1,)), ((), ())), preferred_element_type=F32,
        )
        return both[:width] + both[width:]

    def pairs_of(steps):
        return [step * sides + pair for step in steps for pair in range(sides)]

    def row_copy(tile):
        at = slice(tile * ROW_TILE, (tile + 1) * ROW_TILE)
        return remote(
            total.at[tile], arrived.at[tile], row_send.at[tile], row_recv.at[tile], "rep", partner,
        )

    def alone(work):
        pl.when(me >= 0)(work)

    def stage_step(new, old, whiches=(0, 1)):
        if sides == 1:
            stage(None if new is None else (new, 0), None if old is None else (old, 0), whiches)
        elif old is not None and 1 in whiches:
            for pair in range(sides):
                stage((old, pair), None)
                stage(None, (old, pair))

    def early_rows(steps, add):
        groups = [list(steps)] if sides == 1 else [[step] for step in steps]
        for place, group_steps in enumerate(groups):
            for half in range(2):
                rows = slice(half * rows_out, (half + 1) * rows_out)
                value = grad_rows(half * rows_out, rows_out, pairs_of(group_steps))
                sums[:, rows] = sums[:, rows] + value if add or place else value

    for step in (1, 2, 3, 0) if sides > 1 else (1,):
        wait_ids(step)
    alone(lambda: stage_step(1, None))
    pass_on(1)
    send_far(0)
    for step in (2, 3, 0) if sides == 1 else ():
        wait_ids(step)
    for away in range(1, outer):
        far_id_copy(away).start()
    alone(lambda: stage_step(2, 1))
    start_parts(1)
    alone(lambda: stage_step(3, 2, (0,)))
    pass_on(2)
    send_far(1)
    alone(lambda: stage_step(3, 2, (1,)))
    start_parts(2)
    alone(lambda: stage_step(0, 3, (0,)))
    pass_on(3)
    alone(lambda: stage_step(0, 3, (1,)))
    start_parts(3)
    send_far(2)
    alone(lambda: stage_step(None, 0))
    start_parts(0)
    for away in range(1, outer):
        far_id_copy(away).wait_recv()
    alone(lambda: count_far(0))
    sum_parts(1)
    alone(lambda: count_far(1))
    alone(lambda: count_far(2))
    send_far(3)
    sum_parts(2)
    for step in range(3):
        scale_own(step)
    alone(lambda: early_rows((0, 1, 2), False))
    alone(lambda: count_far(3))
    sum_parts(3)
    for away in range(2, outer):
        for step in range(features):
            count_far(step, away)
    for away in range(1, outer):
        for step in range(2 if away == outer - 1 else features):
            scale_far(away, step)
    scale_own(3)
    alone(lambda: early_rows(range(3, outer * features - 2), True))
    scale_far(outer - 1, 2)
    alone(lambda: early_rows((outer * features - 2,), True))
    sum_parts(0)
    scale_far(outer - 1, 3)
    last = pairs_of((outer * features - 1,))
    tiles = rows_out // ROW_TILE
    start = pl.multiple_of((core + 1) % INNER * rows_out, ROW_TILE)
    value = grad_rows(start, rows_out, last) + sums[:, pl.ds(start, rows_out)]
    for tile in range(tiles):
        total[tile] = value[:, tile * ROW_TILE : (tile + 1) * ROW_TILE]
        row_copy(tile).start()
    start = pl.multiple_of(core * rows_out, ROW_TILE)
    value = grad_rows(start, rows_out, last) + sums[:, pl.ds(start, rows_out)]
    for tile in range(tiles):
        grads[tile] = value[:, tile * ROW_TILE : (tile + 1) * ROW_TILE]
    for step in range(1, features):
        pool_copy(across(step), crossed(step)).wait_recv()
    for tile in range(tiles):
        row_copy(tile).wait_recv()

    for tile in range(tiles):
        row_copy(tile).wait_send()
    for step in range(1, n):
        id_copy(near(step), me).wait_send()
    for side in range(1, owners):
        cot_copy(beside(side), me).wait_send()
    for away in range(1, outer):
        far_id_copy(away).wait_send()
        far_copy(me, away, True).wait_send()
    for step in range(features):
        source = across(step)
        if step:
            cot_copy(source, me).wait_send()
            pool_copy(source, feature).wait_send()
            for away in range(1, outer):
                far_copy(source, away).wait_send()
        for side in range(1, owners):
            if step:
                pass_copy(source, side).wait_send()
            other = source_of(step, side)
            for away in range(1, outer):
                far_copy(other, away).wait_send()
            part_copy(other, crossed(step) * owners + lane).wait_send()


def finish(lens, pool, own, arrived, pooled, grads):
    for at in range(pool.shape[0]):
        pooled[at] = pool[at] * (1.0 / lens[at : at + 1].astype(F32))
    for tile in range(own.shape[0]):
        grads[:, tile * ROW_TILE : (tile + 1) * ROW_TILE] = own[tile] + arrived[tile]


def body(n, reps, emb_table, feature_ids, lengths, cotangent):
    rows_dev, width = emb_table.shape
    each, features, bag = feature_ids.shape
    lens = lengths.T
    owners = n // features
    outer = reps // INNER
    rows_out = rows_dev // reps
    kept = rows_out * INNER
    tiles = rows_out // ROW_TILE
    away = max(outer - 1, 1)
    sem = pltpu.SemaphoreType.DMA
    vmem = pl.BlockSpec(memory_space=pltpu.VMEM)
    pool_shape = jax.ShapeDtypeStruct((features, width, each), F32)
    tile_shape = jax.ShapeDtypeStruct((tiles, width, ROW_TILE), F32)
    scratch = [
        pltpu.VMEM((width, rows_dev), F32),
        pltpu.VMEM((features, bag, each), I32),
        pltpu.VMEM((features, each), I32),
        pltpu.VMEM((features, width, each), F32),
        pltpu.VMEM((features, bag, each), I32),
        sem((4,)),
        pltpu.VMEM((n, bag, each), I32),
        pltpu.VMEM((away, n, bag, each), I32),
        pltpu.VMEM((n, width, each), F32),
        pltpu.VMEM((away, n, width, each), F32),
        pltpu.VMEM((2 * width, rows_dev), BF16),
        pltpu.VMEM((n, width, each), F32),
        pltpu.VMEM((n, width, each), F32),
        pltpu.VMEM((2 * width, outer * n * each), BF16),
        pltpu.VMEM((width, kept), F32),
        pltpu.VMEM((tiles, width, ROW_TILE), F32),
        sem((n,)), sem((n,)), sem((n,)), sem((n,)), sem((features, owners)),
        sem((away, n)), sem((away, n)), sem((away,)), sem((away,)),
        sem((n,)), sem((n,)), sem((features,)), sem((features,)),
        sem((tiles,)), sem((tiles,)),
    ]
    scratch += [pltpu.VMEM((kept, 2 * each), BF16)] * (outer * n // 2)
    scratch += [pltpu.VMEM((rows_dev - kept, 2 * each), BF16)] * 2
    held = [ref for ref in scratch if ref.memory_space == pltpu.VMEM]
    blocks = sum(math.prod(ref.shape) * jnp.dtype(ref.dtype).itemsize for ref in held)
    blocks += 4 * (features * width * each + 2 * width * rows_out)
    limit = min(65000 * 1024, blocks + (12 << 20))
    pool, own, arrived = pl.pallas_call(
        functools.partial(kernel, n, reps),
        out_shape=(pool_shape, tile_shape, tile_shape),
        in_specs=[pl.BlockSpec(memory_space=pltpu.HBM)] * 4,
        out_specs=[vmem] * 3,
        scratch_shapes=scratch,
        compiler_params=pltpu.CompilerParams(
            collective_id=0, has_side_effects=True, vmem_limit_bytes=limit
        ),
    )(
        *(
            pltpu.with_memory_space_constraint(array, pltpu.HBM)
            for array in (
                emb_table.T, jnp.transpose(feature_ids, (1, 2, 0)), lens,
                jnp.transpose(cotangent, (1, 2, 0)),
            )
        )
    )
    pooled, grads = pl.pallas_call(
        finish,
        out_shape=(pool_shape, jax.ShapeDtypeStruct((width, rows_out), F32)),
        in_specs=[vmem] * 4,
        out_specs=[vmem] * 2,
        compiler_params=pltpu.CompilerParams(vmem_limit_bytes=8 << 20),
    )(lens, pool, own, arrived)
    return jnp.transpose(pooled, (2, 0, 1)), grads.T


def solution(mesh):
    return jax.shard_map(
        functools.partial(body, mesh.shape["dev"], mesh.shape["rep"]),
        mesh=mesh,
        in_specs=(
            P("dev", None),
            P(("dev", "rep"), None, None),
            P(("dev", "rep"), None),
            P(("dev", "rep"), None, None),
        ),
        out_specs=(P(("dev", "rep"), None, None), P(("dev", "rep"), None)),
        check_vma=False,
    )
```

```python
import functools
import math

import jax
import jax.numpy as jnp
from jax import lax
from jax.experimental import pallas as pl
from jax.experimental.pallas import tpu as pltpu
from jax.sharding import PartitionSpec as P

F32, BF16, I32, I16 = jnp.float32, jnp.bfloat16, jnp.int32, jnp.int16
ROW_TILE = 256
BLOCK = 64
CHUNK = 512
INNER = 2


def split_bits(value):
    high = value.astype(BF16)
    low = (value - high.astype(F32)).astype(BF16)
    return high, low


def repeat(count, step):
    if count == 1:
        step(0)
    else:
        lax.fori_loop(0, count, lambda at, _: (step(at), 0)[1], 0)


def kernel(
    n, reps, table_in, ids_in, lens_in, cot_in, pool_in, grads, arrived,
    table, raw, lens, cot, ids, stage, ids_buf, peer_ids, cot_buf, peer_cot, halves, part, part_in,
    scaled, sums, total,
    id_send, id_recv, cot_send, cot_recv, pass_send, far_send, far_recv, far_id_send, far_id_recv,
    part_send, part_recv, pool_send, pool_recv, row_send, row_recv, *counted,
):
    features, bag, each = ids.shape
    width, rows_dev = table.shape
    owners = n // features
    outer = reps // INNER
    rows_out = rows_dev // reps
    kept = rows_out * INNER
    me = lax.axis_index("dev")
    rep = lax.axis_index("rep")
    feature = me // owners
    lane = me % owners
    group = rep // INNER
    core = rep % INNER
    first_row = group * kept
    sides = owners // 2
    counts, rests = counted[: outer * n // 2], counted[outer * n // 2 :]
    bits = features.bit_length() - 1

    def crossed(step):
        value = feature
        for bit in range(bits):
            value = value + (step // (1 << bit) % 2) * (1 - 2 * (feature // (1 << bit) % 2)) * (1 << bit)
        return value

    def near(step):
        return (me + step) % n

    def beside(side):
        return feature * owners + (lane + side) % owners

    def across(step):
        return crossed(step) * owners + lane

    def source_of(step, side):
        return crossed(step) * owners + (lane + side) % owners

    def far(step):
        return (group + step) % outer * INNER + core

    partner = group * INNER + (core + 1) % INNER

    barrier = pltpu.get_barrier_semaphore()
    for step in range(1, n):
        pl.semaphore_signal(
            barrier, inc=1, device_id={"dev": near(step)}, device_id_type=pl.DeviceIdType.MESH
        )
    for step in range(1, outer):
        pl.semaphore_signal(
            barrier, inc=1, device_id={"rep": far(step)}, device_id_type=pl.DeviceIdType.MESH
        )
    pl.semaphore_signal(
        barrier, inc=1, device_id={"rep": partner}, device_id_type=pl.DeviceIdType.MESH
    )
    staged = [
        pltpu.make_async_copy(src, dst, stage.at[at])
        for at, (src, dst) in enumerate(
            ((ids_in, raw), (lens_in, lens), (cot_in, cot), (table_in, table))
        )
    ]
    for copy in staged:
        copy.start()
    staged[0].wait()
    staged[1].wait()
    slot_index = lax.broadcasted_iota(I32, (bag, each), 0)
    for at in range(features):
        ids[at] = jnp.where(slot_index < lens[at : at + 1], raw[at], -(1 << 20))
    staged[2].wait()
    ids_buf[me] = ids[feature]
    cot_buf[me] = cot[feature]
    pl.semaphore_wait(barrier, n - 1 + outer)

    def remote(src, dst, send, recv, axis, to):
        return pltpu.make_async_remote_copy(
            src_ref=src, dst_ref=dst, send_sem=send, recv_sem=recv,
            device_id={axis: to}, device_id_type=pl.DeviceIdType.MESH,
        )

    def id_copy(peer, source):
        return remote(
            ids.at[peer // owners], ids_buf.at[source],
            id_send.at[peer], id_recv.at[source], "dev", peer,
        )

    def cot_copy(peer, source):
        return remote(
            cot.at[peer // owners], cot_buf.at[source],
            cot_send.at[peer], cot_recv.at[source], "dev", peer,
        )

    def pass_copy(source, side):
        return remote(
            cot_buf.at[source], cot_buf.at[source],
            pass_send.at[source // owners, side], cot_recv.at[source], "dev", beside(side),
        )

    def far_copy(source, step, own=False):
        return remote(
            cot.at[feature] if own else cot_buf.at[source], peer_cot.at[step - 1, source],
            far_send.at[step - 1, source], far_recv.at[step - 1, source], "rep", far(step),
        )

    def far_id_copy(step):
        return remote(
            ids_buf, peer_ids.at[step - 1],
            far_id_send.at[step - 1], far_id_recv.at[step - 1], "rep", far(step),
        )

    def part_copy(source, slot):
        return remote(
            part.at[source], part_in.at[slot], part_send.at[source], part_recv.at[slot],
            "dev", feature * owners + source % owners,
        )

    def pool_copy(source, slot):
        return remote(
            part.at[source], pool_in.at[slot],
            pool_send.at[source // owners], pool_recv.at[slot], "dev", source,
        )

    for step in range(1, n):
        id_copy(near(step), me).start()
    for step in (1, 3, 2):
        cot_copy(across(step), me).start()
    for side in range(1, owners):
        cot_copy(beside(side), me).start()
    for step in range(1, outer):
        far_copy(me, step, True).start()

    staged[3].wait()

    def split_table(tile):
        at = pl.ds(pl.multiple_of(tile * ROW_TILE, ROW_TILE), ROW_TILE)
        start = (first_row + tile * ROW_TILE) % rows_dev
        high, low = split_bits(table[:, pl.ds(pl.multiple_of(start, ROW_TILE), ROW_TILE)])
        halves[:width, at] = high
        halves[width:, at] = low

    repeat(rows_dev // ROW_TILE, split_table)

    def pass_on(step):
        source = across(step)
        cot_copy(source, source).wait_recv()
        for side in range(1, owners):
            pass_copy(source, side).start()
        for away in range(1, outer):
            far_copy(source, away).start()

    def send_far(step):
        for side in range(1, owners):
            source = source_of(step, side)
            cot_copy(source, source).wait_recv()
            for away in range(1, outer):
                far_copy(source, away).start()

    def slot_keys(blocks, rows):
        slots = jnp.concatenate(blocks, axis=1)
        wide = slots.shape[1]
        local = slots - lane * rows_dev
        turned = local - first_row
        turned = jnp.where(turned < 0, turned + rows_dev, turned)
        inside = (local >= 0) & (local < rows_dev) & (turned < rows)
        keys, times = [], []
        for j in range(bag):
            same = (slots == slots[j : j + 1]).astype(I32)
            count = jnp.sum(same, axis=0, keepdims=True)
            keep = inside[j : j + 1]
            if j:
                keep = keep & (jnp.sum(same[:j], axis=0, keepdims=True) == 0)
            key = jnp.where(keep, turned[j : j + 1], -1)
            keys.append(jnp.broadcast_to(key, (16, wide)).astype(I16))
            times.append(jnp.broadcast_to(count.astype(F32), (16, wide)).astype(BF16))
        return keys, times

    def count_rows(keys, times, start, first, rows, target):
        wide = keys[0].shape[1]
        lanes = wide // 128
        row = lax.broadcasted_iota(I32, (16, 128), 0)
        spread = BLOCK // 16
        keys = [jnp.concatenate([key] * spread, axis=0) for key in keys]
        times = [jnp.concatenate([time] * spread, axis=0) for time in times]

        def count_block(block):
            base = start + block * BLOCK
            here = [(row + (base + 16 * at)).astype(I16) for at in range(spread)]
            here = jnp.concatenate([jnp.concatenate([one] * lanes, axis=1) for one in here], axis=0)
            found = jnp.zeros((BLOCK, wide), BF16)
            for key, time in zip(keys, times):
                found = jnp.where(key == here, time, found)
            at = block * BLOCK
            target[pl.ds(at if sides == 1 else pl.multiple_of(at, BLOCK), BLOCK), :] = found

        if sides == 1:
            for block in range(first // BLOCK, (first + rows) // BLOCK):
                count_block(block)
        else:
            repeat(rows // BLOCK, lambda block: count_block(first // BLOCK + block))

    def wait_ids(step):
        for side in range(owners):
            if step or side:
                source = source_of(step, side)
                id_copy(source, source).wait_recv()

    def pair_at(step, pair, away=0):
        return (away * features + step) * sides + pair

    def keys_of(step, pair):
        return slot_keys([ids_buf[source_of(step, pair * 2 + half)] for half in range(2)], rows_dev)

    def halves_of(at):
        return (counts[at], 0, kept), (rests[at % 2], kept, rows_dev - kept)

    def stage(new, old, whiches=(0, 1)):
        if new is not None:
            keys, times = keys_of(*new)
        pool = None
        for which in whiches:
            rows = (kept, rows_dev - kept)[which]
            for first in range(0, rows, CHUNK):
                if old is not None:
                    target, start, _ = halves_of(pair_at(*old))[which]
                    piece = jnp.dot(
                        halves[:, start + first : start + first + CHUNK], target[first : first + CHUNK, :],
                        preferred_element_type=F32,
                    )
                    pool = piece if pool is None else pool + piece
                if new is not None:
                    target, start, _ = halves_of(pair_at(*new))[which]
                    count_rows(keys, times, start, first, CHUNK, target)
        if old is not None:
            step, pair = old
            pool = pool[:width] + pool[width:]
            for half in range(2):
                source = source_of(step, pair * 2 + half)
                value = pool[:, half * each : (half + 1) * each]
                part[source] = value if 0 in whiches else part[source] + value

    def start_parts(step):
        for side in range(1, owners):
            source = source_of(step, side)
            part_copy(source, source // owners * owners + lane).start()

    def count_far(step, away=1):
        for pair in range(sides):
            blocks = [peer_ids[away - 1, source_of(step, pair * 2 + half)] for half in range(2)]
            keys, times = slot_keys(blocks, kept)
            count_rows(keys, times, 0, 0, kept, counts[pair_at(step, pair, away)])

    def sum_parts(step):
        source = across(step)
        value = part[source]
        for side in range(1, owners):
            slot = source // owners * owners + (lane + side) % owners
            part_copy(source, slot).wait_recv()
            value = value + part_in[slot]
        if step:
            part[source] = value
            pool_copy(source, feature).start()
        else:
            pool_in[feature] = value

    def scale_block(live_ids, block, column):
        live = jnp.sum((live_ids >= 0).astype(F32), axis=0, keepdims=True)
        high, low = split_bits(block * (1.0 / live))
        columns = pl.ds(pl.multiple_of(column * each, each), each)
        scaled[:width, columns] = high
        scaled[width:, columns] = low

    def scale_own(step):
        def one(side):
            source = source_of(step, side)
            scale_block(ids_buf[source], cot_buf[source], step * owners + side)

        repeat(owners, one)

    def scale_far(away, step):
        for side in range(owners):
            source = source_of(step, side)
            far_copy(source, away).wait_recv()
            scale_block(peer_ids[away - 1, source], peer_cot[away - 1, source], away * n + step * owners + side)

    def grad_rows(start, rows, pairs):
        at = pl.ds(pl.multiple_of(start, ROW_TILE), rows)
        left = jnp.concatenate([scaled[:, pair * 2 * each : (pair + 1) * 2 * each] for pair in pairs], axis=1)
        held = jnp.concatenate([counts[pair][at, :] for pair in pairs], axis=1)
        both = lax.dot_general(
            left, held, (((1,), (1,)), ((), ())), preferred_element_type=F32,
        )
        return both[:width] + both[width:]

    def pairs_of(steps):
        return [step * sides + pair for step in steps for pair in range(sides)]

    def row_copy(tile):
        at = slice(tile * ROW_TILE, (tile + 1) * ROW_TILE)
        return remote(
            total.at[tile], arrived.at[tile], row_send.at[tile], row_recv.at[tile], "rep", partner,
        )

    def alone(work):
        pl.when(me >= 0)(work)

    def stage_step(new, old, whiches=(0, 1)):
        if sides == 1:
            stage(None if new is None else (new, 0), None if old is None else (old, 0), whiches)
        elif old is not None and 1 in whiches:
            for pair in range(sides):
                stage((old, pair), None)
                stage(None, (old, pair))

    def mixed(steps, ahead):
        if sides > 1:
            early_rows(steps, False)
            for step in ahead:
                count_far(step)
            return
        part_rows = kept // 4
        keyed = [slot_keys([peer_ids[0, source_of(step, half)] for half in range(2)], kept) for step in ahead]
        for place in range(4):
            rows = slice(place * part_rows, (place + 1) * part_rows)
            sums[:, rows] = grad_rows(place * part_rows, part_rows, pairs_of(steps))
            which = place * len(ahead) // 4
            rows = kept * len(ahead) // 4
            target = counts[pair_at(ahead[which], 0, 1)]
            count_rows(*keyed[which], 0, place * rows - which * kept, rows, target)

    def early_rows(steps, add):
        groups = [list(steps)] if sides == 1 else [[step] for step in steps]
        for place, group_steps in enumerate(groups):
            for half in range(2):
                rows = slice(half * rows_out, (half + 1) * rows_out)
                value = grad_rows(half * rows_out, rows_out, pairs_of(group_steps))
                sums[:, rows] = sums[:, rows] + value if add or place else value

    for step in range(features) if sides > 1 else (1,):
        wait_ids(step)
    alone(lambda: stage_step(1, None))
    pass_on(1)
    send_far(0)
    for step in (2, 3, 0) if sides == 1 else ():
        wait_ids(step)
    for away in range(1, outer):
        far_id_copy(away).start()
    alone(lambda: stage_step(2, 1))
    start_parts(1)
    alone(lambda: stage_step(3, 2, (0,)))
    pass_on(2)
    send_far(1)
    alone(lambda: stage_step(3, 2, (1,)))
    start_parts(2)
    alone(lambda: stage_step(0, 3, (0,)))
    pass_on(3)
    alone(lambda: stage_step(0, 3, (1,)))
    start_parts(3)
    alone(lambda: stage_step(None, 0))
    send_far(2)
    for away in range(1, outer):
        far_id_copy(away).wait_recv()
    alone(lambda: count_far(0))
    sum_parts(1)
    alone(lambda: count_far(1))
    for step in range(3):
        scale_own(step)
    alone(lambda: count_far(2))
    send_far(3)
    start_parts(0)
    sum_parts(2)
    alone(lambda: mixed((0, 1, 2), (3,)))
    for away in range(2, outer):
        for step in range(features):
            count_far(step, away)
    sum_parts(3)
    for away in range(1, outer):
        for step in range(2 if away == outer - 1 else features):
            scale_far(away, step)
    scale_own(3)
    alone(lambda: early_rows(range(3, outer * features - 2), True))
    scale_far(outer - 1, 2)
    scale_far(outer - 1, 3)
    last = pairs_of((outer * features - 2, outer * features - 1))
    tiles = rows_out // ROW_TILE
    start = pl.multiple_of((core + 1) % INNER * rows_out, ROW_TILE)
    value = grad_rows(start, rows_out, last) + sums[:, pl.ds(start, rows_out)]
    for tile in range(tiles):
        total[tile] = value[:, tile * ROW_TILE : (tile + 1) * ROW_TILE]
        row_copy(tile).start()
    start = pl.multiple_of(core * rows_out, ROW_TILE)
    value = grad_rows(start, rows_out, last) + sums[:, pl.ds(start, rows_out)]
    for tile in range(tiles):
        grads[tile] = value[:, tile * ROW_TILE : (tile + 1) * ROW_TILE]
    sum_parts(0)
    for step in range(1, features):
        pool_copy(across(step), crossed(step)).wait_recv()
    for tile in range(tiles):
        row_copy(tile).wait_recv()

    for tile in range(tiles):
        row_copy(tile).wait_send()
    for step in range(1, n):
        id_copy(near(step), me).wait_send()
    for side in range(1, owners):
        cot_copy(beside(side), me).wait_send()
    for away in range(1, outer):
        far_id_copy(away).wait_send()
        far_copy(me, away, True).wait_send()
    for step in range(features):
        source = across(step)
        if step:
            cot_copy(source, me).wait_send()
            pool_copy(source, feature).wait_send()
            for away in range(1, outer):
                far_copy(source, away).wait_send()
        for side in range(1, owners):
            other = source_of(step, side)
            if step:
                pass_copy(source, side).wait_send()
            for away in range(1, outer):
                far_copy(other, away).wait_send()
            part_copy(other, crossed(step) * owners + lane).wait_send()


def finish(lens, pool, own, arrived, pooled, grads):
    for at in range(pool.shape[0]):
        pooled[at] = pool[at] * (1.0 / lens[at : at + 1].astype(F32))
    for tile in range(own.shape[0]):
        grads[:, tile * ROW_TILE : (tile + 1) * ROW_TILE] = own[tile] + arrived[tile]


def body(n, reps, emb_table, feature_ids, lengths, cotangent):
    rows_dev, width = emb_table.shape
    each, features, bag = feature_ids.shape
    lens = lengths.T
    owners = n // features
    outer = reps // INNER
    rows_out = rows_dev // reps
    kept = rows_out * INNER
    tiles = rows_out // ROW_TILE
    away = max(outer - 1, 1)
    sem = pltpu.SemaphoreType.DMA
    vmem = pl.BlockSpec(memory_space=pltpu.VMEM)
    pool_shape = jax.ShapeDtypeStruct((features, width, each), F32)
    tile_shape = jax.ShapeDtypeStruct((tiles, width, ROW_TILE), F32)
    scratch = [
        pltpu.VMEM((width, rows_dev), F32),
        pltpu.VMEM((features, bag, each), I32),
        pltpu.VMEM((features, each), I32),
        pltpu.VMEM((features, width, each), F32),
        pltpu.VMEM((features, bag, each), I32),
        sem((4,)),
        pltpu.VMEM((n, bag, each), I32),
        pltpu.VMEM((away, n, bag, each), I32),
        pltpu.VMEM((n, width, each), F32),
        pltpu.VMEM((away, n, width, each), F32),
        pltpu.VMEM((2 * width, rows_dev), BF16),
        pltpu.VMEM((n, width, each), F32),
        pltpu.VMEM((n, width, each), F32),
        pltpu.VMEM((2 * width, outer * n * each), BF16),
        pltpu.VMEM((width, kept), F32),
        pltpu.VMEM((tiles, width, ROW_TILE), F32),
        sem((n,)), sem((n,)), sem((n,)), sem((n,)), sem((features, owners)),
        sem((away, n)), sem((away, n)), sem((away,)), sem((away,)),
        sem((n,)), sem((n,)), sem((features,)), sem((features,)),
        sem((tiles,)), sem((tiles,)),
    ]
    scratch += [pltpu.VMEM((kept, 2 * each), BF16)] * (outer * n // 2)
    scratch += [pltpu.VMEM((rows_dev - kept, 2 * each), BF16)] * 2
    held = [ref for ref in scratch if ref.memory_space == pltpu.VMEM]
    blocks = sum(math.prod(ref.shape) * jnp.dtype(ref.dtype).itemsize for ref in held)
    blocks += 4 * (features * width * each + 2 * width * rows_out)
    limit = min(65000 * 1024, blocks + (12 << 20))
    pool, own, arrived = pl.pallas_call(
        functools.partial(kernel, n, reps),
        out_shape=(pool_shape, tile_shape, tile_shape),
        in_specs=[pl.BlockSpec(memory_space=pltpu.HBM)] * 4,
        out_specs=[vmem] * 3,
        scratch_shapes=scratch,
        compiler_params=pltpu.CompilerParams(
            collective_id=0, has_side_effects=True, vmem_limit_bytes=limit
        ),
    )(
        *(
            pltpu.with_memory_space_constraint(array, pltpu.HBM)
            for array in (
                emb_table.T, jnp.transpose(feature_ids, (1, 2, 0)), lens,
                jnp.transpose(cotangent, (1, 2, 0)),
            )
        )
    )
    pooled, grads = pl.pallas_call(
        finish,
        out_shape=(pool_shape, jax.ShapeDtypeStruct((width, rows_out), F32)),
        in_specs=[vmem] * 4,
        out_specs=[vmem] * 2,
        compiler_params=pltpu.CompilerParams(vmem_limit_bytes=8 << 20),
    )(lens, pool, own, arrived)
    return jnp.transpose(pooled, (2, 0, 1)), grads.T


def solution(mesh):
    return jax.shard_map(
        functools.partial(body, mesh.shape["dev"], mesh.shape["rep"]),
        mesh=mesh,
        in_specs=(
            P("dev", None),
            P(("dev", "rep"), None, None),
            P(("dev", "rep"), None),
            P(("dev", "rep"), None, None),
        ),
        out_specs=(P(("dev", "rep"), None, None), P(("dev", "rep"), None)),
        check_vma=False,
    )
```
